32 devices in a mesh: grp: 2 (over x), freq: 16 (over z, y, core).
Axes of the slice: x: 2, y: 2, z: 4, core: 2. Of those that a mesh axis runs over, the one named last changes fastest.
Arguments:
- kernel: bfloat16 [2, 256, 1024, 1024], P(None, ('grp', 'freq')), parts along dimension 1, may hold values from -0.125 to 0.125
- recorded: float32 [2, 256, 1024, 128], P(None, ('grp', 'freq')), parts along dimension 1, may hold values from -8 to 8
- onset_time: int32 [2048, 128], P(('grp', 'freq')), parts along dimension 0, may hold values from 32 to 256, as said below
Outputs:
- focusing: float32 [256, 2048, 128], P(None, ('grp', 'freq')), parts along dimension 1
The draws below stay inside these ranges and needn't reach their ends.
There are 2 independent parts, one for each index of `grp`. The reference program is written for one: setup_inputs(seed, part) draws one part's arguments, and reference() takes and returns one part's arrays. A program takes and returns all parts, laid end to end along the dimension named above; each array names one. Nothing has to cross between parts.
Inputs may be any that keep to these rules, and one draw needn't show every extreme that they name: `onset_time`: onset sample of the window for each receiver and focal point.
All inputs are finite; a program needn't handle non-finite values.
Results may differ from the reference program's by a relative error of at most 0.012.
Values may be sent and summed in bfloat16 or wider, within the bound.
A program may use at most 192 MiB of HBM per device.

```python
import math
import jax
import jax.numpy as jnp
from jax import lax

SRC = 1024
REC = 1024
NF = 128
FOCAL = 128
ITERS = 2
NT = 256


def draw_recorded(key, part):
    shape = (2, NF, SRC, FOCAL)
    base = jax.random.normal(jax.random.fold_in(key, 21), shape, jnp.float32)
    column_log = jax.random.uniform(jax.random.fold_in(key, 22), (1, 1, 1, FOCAL), jnp.float32, -2.5, 1.5)
    tilt = jax.random.uniform(jax.random.fold_in(key, 23), (1, 1, 1, FOCAL), jnp.float32, -2.0, 2.0)
    source_log = jax.random.uniform(jax.random.fold_in(key, 24), (1, 1, SRC, 1), jnp.float32, -0.8, 0.8)
    freq_pos = (jnp.arange(NF, dtype=jnp.float32) / NF - 0.5).reshape(1, NF, 1, 1)
    value = base * jnp.exp(column_log + tilt * freq_pos + source_log)
    return jnp.clip(value, -8.0, 8.0).astype(jnp.float32)


def draw_onset_time(key, part):
    rows = jnp.arange(REC, dtype=jnp.int32)[:, None]
    base = NT // 8 + rows * (5 * NT // 8) // REC
    jitter = jax.random.randint(jax.random.fold_in(key, 11), (REC, FOCAL), 0, NT // 4 + 1, dtype=jnp.int32)
    column_shift = jax.random.randint(jax.random.fold_in(key, 12), (1, FOCAL), -(3 * NT // 8), NT // 2 + 1, dtype=jnp.int32)
    onset = jnp.clip(base + jitter + column_shift, NT // 8, NT).astype(jnp.int32)
    onset = onset.at[0, 0].set(NT // 8)
    onset = onset.at[REC - 1, 0].set(NT)
    return onset.astype(jnp.int32)


def shard_levels(rng, shape, split, least, largest):
    factor_of, own = 1.0, jax.random.fold_in(rng, 6)
    for dim, shards_of in split:
        draws = jnp.exp(jax.random.uniform(jax.random.fold_in(own, dim), (shards_of,), jnp.float32, least / len(split), largest / len(split)))
        factor_of = factor_of * jnp.repeat(draws, shape[dim] // shards_of).reshape([-1 if axis == dim else 1 for axis in range(len(shape))])
    return factor_of


def noise(own_key, extent, width, reach, shards=(), held_as=jnp.bfloat16):
    array = jax.random.normal(own_key, extent, jnp.float32) * width
    if len(shards) > 0:
        array = shard_levels(own_key, extent, shards, -0.22, 0.18) * array
    return jnp.clip(array, min=-reach, max=reach).astype(held_as)


def setup_inputs(seed: int = 0, part: int = 0) -> dict:
    seeds = jax.random.split(jax.random.key(seed), 4)
    part_keys = jax.random.split(jax.random.fold_in(seeds[3], part), 4)
    kernel = noise(part_keys[0], (2, NF, SRC, REC), (2 * REC) ** -0.5, 0.125, ((1, 16),))
    recorded = draw_recorded(jax.random.fold_in(jax.random.fold_in(seeds[3], part), 71), part)
    onset_time = draw_onset_time(jax.random.fold_in(jax.random.fold_in(seeds[3], part), 71), part)
    return {"kernel": kernel, "recorded": recorded, "onset_time": onset_time}


def dft_tables():
    samples = jnp.arange(2 * NF, dtype=jnp.int32)
    bins = jnp.arange(NF, dtype=jnp.int32)
    phase = (bins[:, None] * samples[None, :] % (2 * NF)).astype(jnp.float32) * (math.pi / NF)
    factor = 1.0 / math.sqrt(NF)
    return (jnp.cos(phase) * factor, jnp.sin(phase) * factor)

def reference(kernel, recorded, onset_time):
    highest = lax.Precision.HIGHEST
    cosine_table, sin_tab = dft_tables()
    samples = jnp.arange(2 * NF, dtype=jnp.int32)[:, None, None]
    keep_mask = (samples < onset_time[None]).astype(jnp.float32)
    kern_major = jnp.moveaxis(kernel, 1, 0)

    def apply_forward(model):
        flat_part = (model * keep_mask).reshape(2 * NF, -1)
        spec_real = jnp.dot(cosine_table, flat_part, precision=highest)
        spec_imag = -jnp.dot(sin_tab, flat_part, precision=highest)
        spectrum = jnp.stack([spec_real, spec_imag]).reshape(2, NF, REC, FOCAL).astype(jnp.bfloat16)

        def per_freq(pair):
            kern_slab, spectrum_block = pair
            kernel_real = kern_slab[0].astype(jnp.float32)
            kernel_imaginary = kern_slab[1].astype(jnp.float32)
            solution_real = spectrum_block[0].astype(jnp.float32)
            solution_imaginary = spectrum_block[1].astype(jnp.float32)
            y_real = jnp.dot(kernel_real, solution_real, precision=highest) - jnp.dot(kernel_imaginary, solution_imaginary, precision=highest)
            y_imag = jnp.dot(kernel_real, solution_imaginary, precision=highest) + jnp.dot(kernel_imaginary, solution_real, precision=highest)
            return jnp.stack([y_real, y_imag])
        return jnp.moveaxis(lax.map(per_freq, (kern_major, jnp.moveaxis(spectrum, 1, 0))), 0, 1)

    def apply_adjoint(resid):
        rounded = jnp.moveaxis(resid.astype(jnp.bfloat16), 1, 0)

        def per_freq(pair):
            kern_slab, data_slab = pair
            kernel_real = kern_slab[0].astype(jnp.float32)
            kernel_imaginary = kern_slab[1].astype(jnp.float32)
            update_real = data_slab[0].astype(jnp.float32)
            update_imaginary = data_slab[1].astype(jnp.float32)
            z_real = jnp.dot(kernel_real.T, update_real, precision=highest) + jnp.dot(kernel_imaginary.T, update_imaginary, precision=highest)
            z_imag = jnp.dot(kernel_real.T, update_imaginary, precision=highest) - jnp.dot(kernel_imaginary.T, update_real, precision=highest)
            return jnp.stack([z_real, z_imag]).astype(jnp.bfloat16)
        image_low = lax.optimization_barrier(jnp.moveaxis(lax.map(per_freq, (kern_major, rounded)), 0, 1))
        image = image_low.astype(jnp.float32)
        timed = jnp.dot(cosine_table.T, image[0].reshape(NF, -1), precision=highest) - jnp.dot(sin_tab.T, image[1].reshape(NF, -1), precision=highest)
        return timed.reshape(2 * NF, REC, FOCAL) * keep_mask
    beta_now = jnp.sqrt(jnp.sum(recorded * recorded))
    data_vec = recorded / beta_now
    model_raw = apply_adjoint(data_vec)
    alpha_now = jnp.sqrt(jnp.sum(model_raw * model_raw))
    model_vec = model_raw / alpha_now
    search = model_vec
    estimate = jnp.zeros_like(model_vec)
    phibar_now = beta_now
    rhobar_now = alpha_now
    for iteration in range(ITERS):
        data_raw = apply_forward(model_vec) - alpha_now * data_vec
        beta_now = jnp.sqrt(jnp.sum(data_raw * data_raw))
        data_vec = data_raw / beta_now
        model_raw = apply_adjoint(data_vec) - beta_now * model_vec
        alpha_now = jnp.sqrt(jnp.sum(model_raw * model_raw))
        model_vec = model_raw / alpha_now
        rho_now = jnp.sqrt(rhobar_now * rhobar_now + beta_now * beta_now)
        cosine = rhobar_now / rho_now
        sine_part = beta_now / rho_now
        theta_now = sine_part * alpha_now
        rhobar_now = -cosine * alpha_now
        phi_now = cosine * phibar_now
        phibar_now = sine_part * phibar_now
        estimate = estimate + phi_now / rho_now * search
        search = model_vec - theta_now / rho_now * search
    return estimate
```

```python
import functools
import math

import jax
import jax.numpy as jnp
import numpy as np
from jax import lax
from jax.experimental import pallas as pl
from jax.experimental.pallas import tpu as pltpu
from jax.sharding import PartitionSpec as P

MESH = pl.DeviceIdType.MESH
ROW = 16
F32 = jnp.float32
BF16 = jnp.bfloat16


def dft_table(bins_total):
    samples = np.arange(2 * bins_total)
    bins = np.arange(bins_total)
    phase = (bins[:, None] * samples[None, :] % (2 * bins_total)) * (math.pi / bins_total)
    factor = 1.0 / math.sqrt(bins_total)
    both = np.stack([np.cos(phase) * factor, -np.sin(phase) * factor], axis=1)
    return both.reshape(2 * bins_total, 2 * bins_total).astype(np.float32)


def swap_matrix():
    size = ROW * ROW
    matrix = np.zeros((size, size), np.float32)
    for a in range(ROW):
        for b in range(ROW):
            matrix[b * ROW + a, a * ROW + b] = 1.0
    return matrix


def fold(values):
    rows, lanes = values.shape
    return jnp.sum(values.reshape(rows // 8, 8, lanes), axis=0)


def total(part):
    return jnp.sum(jnp.sum(part, axis=0, keepdims=True), axis=1, keepdims=True)


def dot(a, b):
    return jnp.dot(a, b, preferred_element_type=F32)


def body(members, kern_hbm, rec_hbm, onset_ref, to_time_ref, to_freq_ref, swap_ref,
         first_hbm, second_hbm, resid_hbm, coef_ref,
         kern, fbuf, rbuf, sbuf, abuf, field, slot, turned, mid, sums,
         kern_sem, slot_sem, out_sem, field_sem, send_sem, recv_sem, sum_send, sum_recv):
    me = lax.axis_index("freq")
    bins2, receivers, focal = fbuf.shape
    bins = bins2 // 2
    rows_k, rec_local, _ = rbuf.shape
    sources = kern.shape[2]
    blocks = rec_local // ROW
    times = field.shape[1] // ROW
    others = members - 1
    tile_v = min(256, sources)
    tile_i = min(256, receivers)
    group_k = min(4, rows_k // ROW)
    group_r = 4

    def peer(j):
        step = 1 + lax.rem(j + members // 2 - 1, others)
        return lax.rem(me + step, members)

    def kern_copy(f):
        return pltpu.make_async_copy(kern_hbm.at[:, f], kern.at[:, f], kern_sem.at[f])

    def rec_copy(f):
        s = lax.rem(f, 2)
        return pltpu.make_async_copy(rec_hbm.at[:, f], slot.at[s], slot_sem.at[s])

    def resid_in(f):
        s = lax.rem(f, 2)
        return pltpu.make_async_copy(resid_hbm.at[f], slot.at[s], slot_sem.at[s])

    def resid_out(f):
        s = lax.rem(f, 2)
        return pltpu.make_async_copy(slot.at[s], resid_hbm.at[f], out_sem.at[s])

    def field_copy(ib, out):
        return pltpu.make_async_copy(field.at[ib], out.at[ib], field_sem.at[ib])

    def wait_bytes(view, sem):
        pltpu.make_async_copy(view, view, sem).wait()

    def freq_view():
        return fbuf.at[:, pl.ds(0, others * rec_local), :]

    def rec_view():
        return rbuf.at[pl.ds(0, others * bins2), :, :]

    rec_copy(0).start()

    @pl.loop(0, bins)
    def _(f):
        kern_copy(f).start()

    barrier = pltpu.get_barrier_semaphore()

    @pl.loop(0, others)
    def _(j):
        pl.semaphore_signal(barrier, inc=1, device_id={"freq": peer(j)}, device_id_type=MESH)

    pl.semaphore_wait(barrier, others)

    def share(turn, parts):
        for place, part in enumerate(parts):
            sums[turn, me, place] = part

        @pl.loop(0, others)
        def _(j):
            pltpu.make_async_remote_copy(
                src_ref=sums.at[turn, me], dst_ref=sums.at[turn, me],
                send_sem=sum_send.at[turn], recv_sem=sum_recv.at[turn],
                device_id={"freq": peer(j)}, device_id_type=MESH,
            ).start()

    def collect(turn, count):
        wait_bytes(sums.at[turn, pl.ds(0, others)], sum_recv.at[turn])
        wait_bytes(sums.at[turn, pl.ds(0, others)], sum_send.at[turn])
        return [total(jnp.sum(sums[turn, :, place], axis=0)) for place in range(count)]

    def send_images(turn, f):
        @pl.loop(0, others)
        def _(j):
            to = peer(j)
            pltpu.make_async_remote_copy(
                src_ref=fbuf.at[pl.ds(2 * f, 2), pl.ds(pl.multiple_of(to * rec_local, ROW), rec_local), :],
                dst_ref=rbuf.at[pl.ds(me * bins2 + 2 * f, 2), :, :],
                send_sem=send_sem.at[turn], recv_sem=recv_sem.at[turn],
                device_id={"freq": to}, device_id_type=MESH,
            ).start()

    def send_spectra(turn, ib):
        start = pl.multiple_of(me * rec_local + ib * ROW, ROW)

        @pl.loop(0, others)
        def _(j):
            to = peer(j)
            pltpu.make_async_remote_copy(
                src_ref=sbuf.at[pl.ds(to * bins2, bins2), pl.ds(pl.multiple_of(ib * ROW, ROW), ROW), :],
                dst_ref=abuf.at[:, pl.ds(start, ROW), :],
                send_sem=send_sem.at[turn], recv_sem=recv_sem.at[turn],
                device_id={"freq": to}, device_id_type=MESH,
            ).start()

    def turn_over(v, real, imag):
        both = jnp.concatenate([real, imag], axis=1)
        turned[:, pl.ds(v * tile_v, tile_v)] = both.T.astype(BF16)

    def images(f):
        plain = turned[...]
        cross = jnp.concatenate([plain[focal:], -plain[:focal]], axis=0)
        for i in range(receivers // tile_i):
            cols = pl.ds(i * tile_i, tile_i)
            z = dot(plain, kern[0, f, :, cols]) + dot(cross, kern[1, f, :, cols])
            z = z.T.astype(BF16)
            fbuf[2 * f, cols, :] = z[:, :focal]
            fbuf[2 * f + 1, cols, :] = z[:, focal:]
        mine = pl.ds(pl.multiple_of(me * rec_local, ROW), rec_local)
        rbuf[pl.ds(me * bins2 + 2 * f, 2), :, :] = fbuf[pl.ds(2 * f, 2), mine, :]

    def forward(f, finish, carry):
        real, imag = abuf[2 * f], abuf[2 * f + 1]
        plain = jnp.concatenate([real, imag], axis=1)
        cross = jnp.concatenate([-imag, real], axis=1)
        for v in range(sources // tile_v):
            rows = pl.ds(v * tile_v, tile_v)
            y = dot(kern[0, f, rows, :], plain) + dot(kern[1, f, rows, :], cross)
            carry = finish(v, rows, y[:, :focal], y[:, focal:], carry)
        return carry

    def receivers_side(turn, ib, make_field, carry):
        here = pl.ds(pl.multiple_of(ib * ROW, ROW), ROW)

        @pl.loop(0, rows_k // (ROW * group_k))
        def _(g):
            pieces = []
            for n in range(group_k):
                at = pl.ds((g * group_k + n) * ROW, ROW)
                pieces.append(rbuf[at, here, :].reshape(ROW * ROW, focal))
            out = dot(swap_ref[...], jnp.concatenate(pieces, axis=1)).astype(BF16)
            for n in range(group_k):
                at = pl.ds(pl.multiple_of((g * group_k + n) * ROW, ROW), ROW)
                mid[:, at, :] = out[:, n * focal:(n + 1) * focal].reshape(ROW, ROW, focal)

        steps = lax.broadcasted_iota(jnp.int32, (times, focal), 0)

        def group(g, carry):
            stack = jnp.concatenate([mid[g * group_r + n] for n in range(group_r)], axis=1)
            raw = dot(to_time_ref[...], stack)
            lows = []
            for n in range(group_r):
                r = g * group_r + n
                onset = onset_ref[pl.ds(ib * ROW + r, 1), :]
                kept = jnp.where(steps < onset, raw[:, n * focal:(n + 1) * focal], 0.0)
                kept = make_field(ib, r, kept)
                carry = carry + fold(kept * kept)
                field[ib, pl.ds(r, times, stride=ROW), :] = kept
                lows.append(kept.astype(BF16))
            spec = dot(to_freq_ref[...], jnp.concatenate(lows, axis=1)).astype(BF16)
            for n in range(group_r):
                mid[g * group_r + n] = spec[:, n * focal:(n + 1) * focal]
            return carry

        carry = lax.fori_loop(0, ROW // group_r, group, carry)

        @pl.loop(0, rows_k // (ROW * group_k))
        def _(g):
            pieces = []
            for n in range(group_k):
                at = pl.ds(pl.multiple_of((g * group_k + n) * ROW, ROW), ROW)
                pieces.append(mid[:, at, :].reshape(ROW * ROW, focal))
            out = dot(swap_ref[...], jnp.concatenate(pieces, axis=1)).astype(BF16)
            for n in range(group_k):
                at = pl.ds((g * group_k + n) * ROW, ROW)
                sbuf[at, here, :] = out[:, n * focal:(n + 1) * focal].reshape(ROW, ROW, focal)

        send_spectra(turn, ib)
        start = pl.multiple_of(me * rec_local + ib * ROW, ROW)
        abuf[:, pl.ds(start, ROW), :] = sbuf[pl.ds(me * bins2, bins2), here, :]
        return carry

    zero = jnp.zeros((8, focal), F32)

    def start_step(f, carry):
        @pl.when(f + 1 < bins)
        def _():
            rec_copy(f + 1).start()

        rec_copy(f).wait()
        kern_copy(f).wait()
        s = lax.rem(f, 2)
        for v in range(sources // tile_v):
            rows = pl.ds(v * tile_v, tile_v)
            real, imag = slot[s, 0, rows, :], slot[s, 1, rows, :]
            carry = carry + fold(real * real) + fold(imag * imag)
            turn_over(v, real, imag)
        images(f)
        send_images(0, f)
        return carry

    sum_b = lax.fori_loop(0, bins, start_step, zero)
    rec_copy(0).start()
    wait_bytes(rec_view(), recv_sem.at[0])

    def first_block(ib, carry):
        carry = receivers_side(1, ib, lambda ib, r, kept: kept, carry)
        field_copy(ib, first_hbm).start()
        return carry

    sum_z = lax.fori_loop(0, blocks, first_block, zero)
    share(0, [sum_b, sum_z])
    wait_bytes(freq_view(), send_sem.at[0])
    square_b, square_z = collect(0, 2)
    beta = jnp.sqrt(square_b)
    image_norm = jnp.sqrt(square_z)
    alpha = image_norm / beta
    scale = 1.0 / image_norm
    weight = alpha / beta

    wait_bytes(freq_view(), recv_sem.at[1])
    wait_bytes(rec_view(), send_sem.at[1])

    def middle_step(f, carry):
        @pl.when(f >= 1)
        def _():
            resid_out(f - 1).wait()

        @pl.when(f + 1 < bins)
        def _():
            rec_copy(f + 1).start()

        rec_copy(f).wait()
        s = lax.rem(f, 2)

        def finish(v, rows, real, imag, carry):
            real = real * scale - weight * slot[s, 0, rows, :]
            imag = imag * scale - weight * slot[s, 1, rows, :]
            slot[s, 0, rows, :] = real
            slot[s, 1, rows, :] = imag
            turn_over(v, real, imag)
            return carry + fold(real * real) + fold(imag * imag)

        carry = forward(f, finish, carry)
        resid_out(f).start()
        images(f)
        send_images(2, f)
        return carry

    sum_u = lax.fori_loop(0, bins, middle_step, zero)
    share(1, [sum_u])
    resid_out(bins - 1).wait()
    resid_in(0).start()
    (square_u,) = collect(1, 1)
    beta_u = jnp.sqrt(square_u)
    data_scale = 1.0 / beta_u
    back = beta_u * scale

    wait_bytes(rec_view(), recv_sem.at[2])
    wait_bytes(freq_view(), send_sem.at[2])

    def second_block(ib, carry):
        field_copy(ib, first_hbm).wait()

        def make_field(ib, r, kept):
            return kept * data_scale - back * field[ib, pl.ds(r, times, stride=ROW), :]

        carry = receivers_side(3, ib, make_field, carry)
        field_copy(ib, second_hbm).start()
        return carry

    sum_v = lax.fori_loop(0, blocks, second_block, zero)
    share(2, [sum_v])
    (square_v,) = collect(2, 1)
    alpha_v = jnp.sqrt(square_v)
    last_scale = 1.0 / alpha_v
    last_weight = alpha_v * data_scale

    wait_bytes(freq_view(), recv_sem.at[3])
    wait_bytes(rec_view(), send_sem.at[3])

    def last_step(f, carry):
        @pl.when(f + 1 < bins)
        def _():
            resid_in(f + 1).start()

        resid_in(f).wait()
        s = lax.rem(f, 2)

        def finish(v, rows, real, imag, carry):
            real = real * last_scale - last_weight * slot[s, 0, rows, :]
            imag = imag * last_scale - last_weight * slot[s, 1, rows, :]
            return carry + fold(real * real) + fold(imag * imag)

        return forward(f, finish, carry)

    sum_last = lax.fori_loop(0, bins, last_step, zero)
    share(3, [sum_last])

    @pl.loop(0, blocks)
    def _(ib):
        field_copy(ib, second_hbm).wait()

    (square_last,) = collect(3, 1)

    rho = jnp.sqrt(alpha * alpha + square_u)
    cosine, sine = alpha / rho, beta_u / rho
    phi = cosine * beta
    phibar = sine * beta
    theta = sine * alpha_v
    rhobar = -cosine * alpha_v
    rho_last = jnp.sqrt(rhobar * rhobar + square_last)
    step_last = rhobar / rho_last * phibar / rho_last
    on_first = (phi / rho - step_last * theta / rho) * scale
    on_second = step_last * last_scale
    coef_ref[0] = jnp.broadcast_to(on_first, (8, focal))
    coef_ref[1] = jnp.broadcast_to(on_second, (8, focal))


def make_step(mesh):
    members = mesh.shape["freq"]

    def step(kernel, recorded, onset_time):
        _, bins, sources, receivers = kernel.shape
        rec_local, focal = onset_time.shape
        times = 2 * bins * members
        blocks = rec_local // ROW
        table = dft_table(bins * members)
        any_space = pl.BlockSpec(memory_space=pl.ANY)
        vmem = pl.BlockSpec(memory_space=pltpu.VMEM)
        shape = jax.ShapeDtypeStruct
        first, second, _, coef = pl.pallas_call(
            functools.partial(body, members),
            out_shape=(
                shape((blocks, times * ROW, focal), F32),
                shape((blocks, times * ROW, focal), F32),
                shape((bins, 2, sources, focal), F32),
                shape((2, 8, focal), F32),
            ),
            in_specs=[any_space, any_space, vmem, vmem, vmem, vmem],
            out_specs=(any_space, any_space, any_space, vmem),
            scratch_shapes=[
                pltpu.VMEM((2, bins, sources, receivers), BF16),
                pltpu.VMEM((2 * bins, receivers, focal), BF16),
                pltpu.VMEM((times, rec_local, focal), BF16),
                pltpu.VMEM((times, rec_local, focal), BF16),
                pltpu.VMEM((2 * bins, receivers, focal), BF16),
                pltpu.VMEM((blocks, times * ROW, focal), F32),
                pltpu.VMEM((2, 2, sources, focal), F32),
                pltpu.VMEM((2 * focal, sources), BF16),
                pltpu.VMEM((ROW, times, focal), BF16),
                pltpu.VMEM((4, members, 2, 8, focal), F32),
                pltpu.SemaphoreType.DMA((bins,)),
                pltpu.SemaphoreType.DMA((2,)),
                pltpu.SemaphoreType.DMA((2,)),
                pltpu.SemaphoreType.DMA((blocks,)),
                pltpu.SemaphoreType.DMA((4,)),
                pltpu.SemaphoreType.DMA((4,)),
                pltpu.SemaphoreType.DMA((4,)),
                pltpu.SemaphoreType.DMA((4,)),
            ],
            compiler_params=pltpu.CompilerParams(
                collective_id=0, has_side_effects=True, vmem_limit_bytes=67043328
            ),
            name="lsqr",
        )(
            kernel, recorded, onset_time,
            jnp.asarray(table.T, BF16), jnp.asarray(table, BF16), jnp.asarray(swap_matrix(), BF16),
        )
        both = coef[0, 0, 0] * first + coef[1, 0, 0] * second
        both = both.reshape(blocks, times, ROW, focal).transpose(1, 0, 2, 3)
        return both.reshape(times, rec_local, focal)

    return step


def solution(mesh):
    placed = (
        P(None, ("grp", "freq"), None, None),
        P(None, ("grp", "freq"), None, None),
        P(("grp", "freq"), None),
    )
    return jax.shard_map(
        make_step(mesh), mesh=mesh, in_specs=placed, out_specs=P(None, ("grp", "freq"), None), check_vma=False
    )
```

```python
import functools
import math

import jax
import jax.numpy as jnp
from jax import lax
from jax.experimental import pallas as pl
from jax.experimental.pallas import tpu as pltpu
from jax.sharding import PartitionSpec as P

MESH = pl.DeviceIdType.MESH
ROW = 16
DEPTH = 3
VMEM_MAIN = 36 * 2**20
VMEM_WEIGH = 12 * 2**20
F32 = jnp.float32
BF16 = jnp.bfloat16


def fill_tables(to_time_ref, to_freq_ref, swap_ref):
    times = to_freq_ref.shape[0]
    row = lax.broadcasted_iota(jnp.int32, (times, times), 0)
    sample = lax.broadcasted_iota(jnp.int32, (times, times), 1)
    turn = lax.rem(lax.div(row, 2) * sample + lax.rem(row, 2) * (times // 4), times)
    factor = 1.0 / math.sqrt(times // 2)
    table = jnp.cos(turn.astype(F32) * (2.0 * math.pi / times)) * factor
    to_freq_ref[...] = table.astype(BF16)
    to_time_ref[...] = table.T.astype(BF16)
    size = ROW * ROW
    row = lax.broadcasted_iota(jnp.int32, (size, size), 0)
    column = lax.broadcasted_iota(jnp.int32, (size, size), 1)
    target = lax.rem(row, ROW) * ROW + lax.div(row, ROW)
    swap_ref[...] = jnp.where(column == target, 1.0, 0.0).astype(BF16)


def fold(values):
    rows, lanes = values.shape
    return jnp.sum(values.reshape(rows // 8, 8, lanes), axis=0)


def total(part):
    return jnp.sum(jnp.sum(part, axis=0, keepdims=True), axis=1, keepdims=True)


def dot(a, b):
    return jnp.dot(a, b, preferred_element_type=F32)


def body(members, kern_hbm, rec_hbm, onset_ref,
         first_ref, second_ref, resid_hbm, coef_ref,
         kern, fbuf, rbuf, sbuf, abuf, slot, turned, mid, sums,
         to_time_ref, to_freq_ref, swap_ref,
         kern_sem, slot_sem, out_sem, image_send, image_recv, spec_send, early_recv, last_recv,
         sum_send, sum_recv):
    me = lax.axis_index("freq")
    bins2, receivers, focal = fbuf.shape
    bins = bins2 // 2
    rows_k, rec_local, _ = rbuf.shape
    sources = kern.shape[2]
    blocks = rec_local // ROW
    times = first_ref.shape[1] // ROW
    chunks = 2 if blocks % 2 == 0 else 1
    per_chunk = blocks // chunks
    part = per_chunk * ROW
    others = members - 1
    tile_v = min(256, sources)
    tile_i = min(256, receivers)
    group_k = min(4, rows_k // ROW)
    group_r = 4

    def peer(j):
        step = 1 + lax.rem(j + members // 2 - 1, others)
        return lax.rem(me + step, members)

    def kern_copy(g):
        s = lax.rem(g, DEPTH)
        return pltpu.make_async_copy(kern_hbm.at[:, lax.rem(g, bins)], kern.at[s], kern_sem.at[s])

    def kern_step(g):
        @pl.when(g + DEPTH - 1 < 3 * bins)
        def _():
            kern_copy(g + DEPTH - 1).start()

        kern_copy(g).wait()
        return lax.rem(g, DEPTH)

    def rec_copy(f):
        s = lax.rem(f, 2)
        return pltpu.make_async_copy(rec_hbm.at[:, f], slot.at[s], slot_sem.at[s])

    def resid_in(f):
        s = lax.rem(f, 2)
        return pltpu.make_async_copy(resid_hbm.at[f], slot.at[s], slot_sem.at[s])

    def resid_out(f):
        s = lax.rem(f, 2)
        return pltpu.make_async_copy(slot.at[s], resid_hbm.at[f], out_sem.at[s])

    def wait_bytes(view, sem):
        pltpu.make_async_copy(view, view, sem).wait()

    def image_bytes():
        return rbuf.at[pl.ds(0, others * bins2), pl.ds(0, part), :]

    def spectra_bytes(count, rows):
        return abuf.at[pl.ds(0, count), pl.ds(0, others * rows), :]

    rec_copy(0).start()
    kern_copy(0).start()

    barrier = pltpu.get_barrier_semaphore()

    @pl.loop(0, others)
    def _(j):
        pl.semaphore_signal(barrier, inc=1, device_id={"freq": peer(j)}, device_id_type=MESH)

    def share(turn, parts):
        for place, part in enumerate(parts):
            sums[turn, me, place] = part

        @pl.loop(0, others)
        def _(j):
            pltpu.make_async_remote_copy(
                src_ref=sums.at[turn, me], dst_ref=sums.at[turn, me],
                send_sem=sum_send.at[turn], recv_sem=sum_recv.at[turn],
                device_id={"freq": peer(j)}, device_id_type=MESH,
            ).start()

    def collect(turn, count):
        wait_bytes(sums.at[turn, pl.ds(0, others)], sum_recv.at[turn])
        wait_bytes(sums.at[turn, pl.ds(0, others)], sum_send.at[turn])
        return [total(jnp.sum(sums[turn, :, place], axis=0)) for place in range(count)]

    def send_images(turn, c, first, count):
        @pl.loop(0, others)
        def _(j):
            to = peer(j)
            pltpu.make_async_remote_copy(
                src_ref=fbuf.at[pl.ds(first, count), pl.ds(pl.multiple_of(to * rec_local + c * part, ROW), part), :],
                dst_ref=rbuf.at[pl.ds(me * bins2 + first, count), pl.ds(c * part, part), :],
                send_sem=image_send.at[turn], recv_sem=image_recv.at[turn, c],
                device_id={"freq": to}, device_id_type=MESH,
            ).start()

    def send_spectra(turn, first, count, row, rows, recv):
        @pl.loop(0, others)
        def _(j):
            to = peer(j)
            pltpu.make_async_remote_copy(
                src_ref=sbuf.at[pl.ds(to * bins2 + first, count), pl.ds(pl.multiple_of(row, ROW), rows), :],
                dst_ref=abuf.at[pl.ds(first, count), pl.ds(pl.multiple_of(me * rec_local + row, ROW), rows), :],
                send_sem=spec_send.at[turn], recv_sem=recv,
                device_id={"freq": to}, device_id_type=MESH,
            ).start()

    def send_last(turn):
        @pl.loop(0, bins)
        def _(f):
            send_spectra(turn, 2 * f, 2, (chunks - 1) * part, part, last_recv.at[turn, f])

    def send_rest(turn):
        for c in range(1, chunks):
            send_images(turn, c, 0, bins2)

    def turn_over(v, real, imag):
        both = jnp.concatenate([real, imag], axis=1)
        turned[:, pl.ds(v * tile_v, tile_v)] = both.T.astype(BF16)

    def images(f, k):
        plain = turned[...]
        cross = jnp.concatenate([plain[focal:], -plain[:focal]], axis=0)
        for i in range(receivers // tile_i):
            cols = pl.ds(i * tile_i, tile_i)
            z = dot(plain, kern[k, 0, :, cols]) + dot(cross, kern[k, 1, :, cols])
            z = z.T.astype(BF16)
            fbuf[2 * f, cols, :] = z[:, :focal]
            fbuf[2 * f + 1, cols, :] = z[:, focal:]
        mine = pl.ds(pl.multiple_of(me * rec_local, ROW), rec_local)
        rbuf[pl.ds(me * bins2 + 2 * f, 2), :, :] = fbuf[pl.ds(2 * f, 2), mine, :]

    def forward(f, k, finish, carry):
        real, imag = abuf[2 * f], abuf[2 * f + 1]
        plain = jnp.concatenate([real, imag], axis=1)
        cross = jnp.concatenate([-imag, real], axis=1)
        for v in range(sources // tile_v):
            rows = pl.ds(v * tile_v, tile_v)
            y = dot(kern[k, 0, rows, :], plain) + dot(kern[k, 1, rows, :], cross)
            carry = finish(v, rows, y[:, :focal], y[:, focal:], carry)
        return carry

    def receivers_side(turn, ib, field, make_field, carry):
        here = pl.ds(pl.multiple_of(ib * ROW, ROW), ROW)

        @pl.when(lax.rem(ib, per_chunk) == 0)
        def _():
            wait_bytes(image_bytes(), image_recv.at[turn, lax.div(ib, per_chunk)])

        @pl.loop(0, rows_k // (ROW * group_k))
        def _(g):
            pieces = []
            for n in range(group_k):
                at = pl.ds((g * group_k + n) * ROW, ROW)
                pieces.append(rbuf[at, here, :].reshape(ROW * ROW, focal))
            out = dot(swap_ref[...], jnp.concatenate(pieces, axis=1)).astype(BF16)
            for n in range(group_k):
                at = pl.ds(pl.multiple_of((g * group_k + n) * ROW, ROW), ROW)
                mid[:, at, :] = out[:, n * focal:(n + 1) * focal].reshape(ROW, ROW, focal)

        steps = lax.broadcasted_iota(jnp.int32, (times, focal), 0)

        def group(g, carry):
            stack = jnp.concatenate([mid[g * group_r + n] for n in range(group_r)], axis=1)
            raw = dot(to_time_ref[...], stack)
            lows = []
            for n in range(group_r):
                r = g * group_r + n
                onset = onset_ref[pl.ds(ib * ROW + r, 1), :]
                kept = jnp.where(steps < onset, raw[:, n * focal:(n + 1) * focal], 0.0)
                kept = make_field(ib, r, kept)
                carry = carry + fold(kept * kept)
                field[ib, pl.ds(r, times, stride=ROW), :] = kept
                lows.append(kept.astype(BF16))
            spec = dot(to_freq_ref[...], jnp.concatenate(lows, axis=1)).astype(BF16)
            for n in range(group_r):
                mid[g * group_r + n] = spec[:, n * focal:(n + 1) * focal]
            return carry

        carry = lax.fori_loop(0, ROW // group_r, group, carry)

        @pl.loop(0, rows_k // (ROW * group_k))
        def _(g):
            pieces = []
            for n in range(group_k):
                at = pl.ds(pl.multiple_of((g * group_k + n) * ROW, ROW), ROW)
                pieces.append(mid[:, at, :].reshape(ROW * ROW, focal))
            out = dot(swap_ref[...], jnp.concatenate(pieces, axis=1)).astype(BF16)
            for n in range(group_k):
                at = pl.ds((g * group_k + n) * ROW, ROW)
                sbuf[at, here, :] = out[:, n * focal:(n + 1) * focal].reshape(ROW, ROW, focal)

        if chunks > 1:
            @pl.when(ib < blocks - per_chunk)
            def _():
                send_spectra(turn, 0, bins2, ib * ROW, ROW, early_recv.at[turn])

        start = pl.multiple_of(me * rec_local + ib * ROW, ROW)
        abuf[:, pl.ds(start, ROW), :] = sbuf[pl.ds(me * bins2, bins2), here, :]
        return carry

    zero = jnp.zeros((8, focal), F32)

    def start_step(f, carry):
        @pl.when(f + 1 < bins)
        def _():
            rec_copy(f + 1).start()

        rec_copy(f).wait()

        @pl.when(f == 0)
        def _():
            for g in range(1, DEPTH - 1):
                kern_copy(g).start()

        s = lax.rem(f, 2)
        for v in range(sources // tile_v):
            rows = pl.ds(v * tile_v, tile_v)
            real, imag = slot[s, 0, rows, :], slot[s, 1, rows, :]
            carry = carry + fold(real * real) + fold(imag * imag)
            turn_over(v, real, imag)
        images(f, kern_step(f))

        @pl.when(f == 0)
        def _():
            pl.semaphore_wait(barrier, others)

        send_images(0, 0, 2 * f, 2)
        return carry

    sum_b = lax.fori_loop(0, bins, start_step, zero)
    rec_copy(0).start()
    send_rest(0)
    fill_tables(to_time_ref, to_freq_ref, swap_ref)

    def first_block(ib, carry):
        return receivers_side(0, ib, first_ref, lambda ib, r, kept: kept, carry)

    sum_z = lax.fori_loop(0, blocks, first_block, zero)
    share(0, [sum_b, sum_z])
    send_last(0)
    wait_bytes(fbuf.at[:, pl.ds(0, others * rec_local), :], image_send.at[0])
    square_b, square_z = collect(0, 2)
    beta = jnp.sqrt(square_b)
    image_norm = jnp.sqrt(square_z)
    alpha = image_norm / beta
    scale = 1.0 / image_norm
    weight = alpha / beta

    if chunks > 1:
        wait_bytes(spectra_bytes(bins2, rec_local - part), early_recv.at[0])

    def middle_step(f, carry):
        @pl.when(f >= 1)
        def _():
            resid_out(f - 1).wait()

        @pl.when(f + 1 < bins)
        def _():
            rec_copy(f + 1).start()

        rec_copy(f).wait()
        s = lax.rem(f, 2)

        def finish(v, rows, real, imag, carry):
            real = real * scale - weight * slot[s, 0, rows, :]
            imag = imag * scale - weight * slot[s, 1, rows, :]
            slot[s, 0, rows, :] = real
            slot[s, 1, rows, :] = imag
            turn_over(v, real, imag)
            return carry + fold(real * real) + fold(imag * imag)

        wait_bytes(spectra_bytes(2, part), last_recv.at[0, f])
        k = kern_step(bins + f)
        carry = forward(f, k, finish, carry)
        resid_out(f).start()
        images(f, k)
        send_images(1, 0, 2 * f, 2)
        return carry

    sum_u = lax.fori_loop(0, bins, middle_step, zero)
    share(1, [sum_u])
    send_rest(1)
    resid_out(bins - 1).wait()
    resid_in(0).start()
    (square_u,) = collect(1, 1)
    beta_u = jnp.sqrt(square_u)
    data_scale = 1.0 / beta_u
    back = beta_u * scale

    wait_bytes(sbuf.at[pl.ds(0, others * bins2)], spec_send.at[0])

    def second_block(ib, carry):
        def make_field(ib, r, kept):
            return kept * data_scale - back * first_ref[ib, pl.ds(r, times, stride=ROW), :]

        return receivers_side(1, ib, second_ref, make_field, carry)

    sum_v = lax.fori_loop(0, blocks, second_block, zero)
    share(2, [sum_v])
    send_last(1)
    (square_v,) = collect(2, 1)
    alpha_v = jnp.sqrt(square_v)
    last_scale = 1.0 / alpha_v
    last_weight = alpha_v * data_scale

    if chunks > 1:
        wait_bytes(spectra_bytes(bins2, rec_local - part), early_recv.at[1])

    def last_step(f, carry):
        @pl.when(f + 1 < bins)
        def _():
            resid_in(f + 1).start()

        resid_in(f).wait()
        s = lax.rem(f, 2)

        def finish(v, rows, real, imag, carry):
            real = real * last_scale - last_weight * slot[s, 0, rows, :]
            imag = imag * last_scale - last_weight * slot[s, 1, rows, :]
            return carry + fold(real * real) + fold(imag * imag)

        wait_bytes(spectra_bytes(2, part), last_recv.at[1, f])
        return forward(f, kern_step(2 * bins + f), finish, carry)

    sum_last = lax.fori_loop(0, bins, last_step, zero)
    share(3, [sum_last])

    wait_bytes(fbuf.at[:, pl.ds(0, others * rec_local), :], image_send.at[1])
    wait_bytes(sbuf.at[pl.ds(0, others * bins2)], spec_send.at[1])

    (square_last,) = collect(3, 1)

    rho = jnp.sqrt(alpha * alpha + square_u)
    cosine, sine = alpha / rho, beta_u / rho
    phi = cosine * beta
    phibar = sine * beta
    theta = sine * alpha_v
    rhobar = -cosine * alpha_v
    rho_last = jnp.sqrt(rhobar * rhobar + square_last)
    step_last = rhobar / rho_last * phibar / rho_last
    on_first = (phi / rho - step_last * theta / rho) * scale
    on_second = step_last * last_scale
    coef_ref[0] = jnp.broadcast_to(on_first, (8, focal))
    coef_ref[1] = jnp.broadcast_to(on_second, (8, focal))


def weigh(coef_ref, first_ref, second_ref, out_hbm, held, sem):
    pieces, span = held.shape[0], held.shape[1]
    blocks, _, focal = first_ref.shape
    on_first, on_second = coef_ref[0, 0:1, :], coef_ref[1, 0:1, :]

    def write(n):
        return pltpu.make_async_copy(held.at[n], out_hbm.at[pl.ds(n * span, span)], sem.at[n])

    @pl.loop(0, pieces)
    def _(n):
        rows = pl.ds(pl.multiple_of(n * span * ROW, ROW), span * ROW)
        for ib in range(blocks):
            both = on_first * first_ref[ib, rows, :] + on_second * second_ref[ib, rows, :]
            held[n, :, ib * ROW:(ib + 1) * ROW, :] = both.reshape(span, ROW, focal)
        write(n).start()

    @pl.loop(0, pieces)
    def _(n):
        write(n).wait()


def make_step(mesh):
    members = mesh.shape["freq"]

    def step(kernel, recorded, onset_time):
        _, bins, sources, receivers = kernel.shape
        rec_local, focal = onset_time.shape
        times = 2 * bins * members
        blocks = rec_local // ROW
        hbm = pl.BlockSpec(memory_space=pltpu.HBM)
        vmem = pl.BlockSpec(memory_space=pltpu.VMEM)
        shape = jax.ShapeDtypeStruct
        first, second, _, coef = pl.pallas_call(
            functools.partial(body, members),
            out_shape=(
                shape((blocks, times * ROW, focal), F32),
                shape((blocks, times * ROW, focal), F32),
                shape((bins, 2, sources, focal), F32),
                shape((2, 8, focal), F32),
            ),
            in_specs=[hbm, hbm, vmem],
            out_specs=(vmem, vmem, hbm, vmem),
            scratch_shapes=[
                pltpu.VMEM((DEPTH, 2, sources, receivers), BF16),
                pltpu.VMEM((2 * bins, receivers, focal), BF16),
                pltpu.VMEM((times, rec_local, focal), BF16),
                pltpu.VMEM((times, rec_local, focal), BF16),
                pltpu.VMEM((2 * bins, receivers, focal), BF16),
                pltpu.VMEM((2, 2, sources, focal), F32),
                pltpu.VMEM((2 * focal, sources), BF16),
                pltpu.VMEM((ROW, times, focal), BF16),
                pltpu.VMEM((4, members, 2, 8, focal), F32),
                pltpu.VMEM((times, times), BF16),
                pltpu.VMEM((times, times), BF16),
                pltpu.VMEM((ROW * ROW, ROW * ROW), BF16),
                pltpu.SemaphoreType.DMA((DEPTH,)),
                pltpu.SemaphoreType.DMA((2,)),
                pltpu.SemaphoreType.DMA((2,)),
                pltpu.SemaphoreType.DMA((2,)),
                pltpu.SemaphoreType.DMA((2, 2)),
                pltpu.SemaphoreType.DMA((2,)),
                pltpu.SemaphoreType.DMA((2,)),
                pltpu.SemaphoreType.DMA((2, bins)),
                pltpu.SemaphoreType.DMA((4,)),
                pltpu.SemaphoreType.DMA((4,)),
            ],
            compiler_params=pltpu.CompilerParams(
                collective_id=0, has_side_effects=True, vmem_limit_bytes=VMEM_MAIN
            ),
            name="lsqr",
        )(kernel, recorded, onset_time)
        pieces = 16
        span = times // pieces
        return pl.pallas_call(
            weigh,
            out_shape=shape((times, rec_local, focal), F32),
            in_specs=[vmem, vmem, vmem],
            out_specs=hbm,
            scratch_shapes=[
                pltpu.VMEM((pieces, span, rec_local, focal), F32),
                pltpu.SemaphoreType.DMA((pieces,)),
            ],
            compiler_params=pltpu.CompilerParams(vmem_limit_bytes=VMEM_WEIGH),
            name="weigh",
        )(coef, first, second)

    return step


def solution(mesh):
    placed = (
        P(None, ("grp", "freq"), None, None),
        P(None, ("grp", "freq"), None, None),
        P(("grp", "freq"), None),
    )
    return jax.shard_map(
        make_step(mesh), mesh=mesh, in_specs=placed, out_specs=P(None, ("grp", "freq"), None), check_vma=False
    )
```

```python
import functools
import math

import jax
import jax.numpy as jnp
from jax import lax
from jax.experimental import pallas as pl
from jax.experimental.pallas import tpu as pltpu
from jax.sharding import PartitionSpec as P

MESH = pl.DeviceIdType.MESH
ROW = 16
DEPTH = 3
VMEM_MAIN = 36 * 2**20
VMEM_WEIGH = 12 * 2**20
F32 = jnp.float32
BF16 = jnp.bfloat16


def fill_tables(to_time_ref, to_freq_ref, swap_ref):
    times = to_freq_ref.shape[0]
    row = lax.broadcasted_iota(jnp.int32, (times, times), 0)
    sample = lax.broadcasted_iota(jnp.int32, (times, times), 1)
    turn = lax.rem(lax.div(row, 2) * sample + lax.rem(row, 2) * (times // 4), times)
    factor = 1.0 / math.sqrt(times // 2)
    table = jnp.cos(turn.astype(F32) * (2.0 * math.pi / times)) * factor
    to_freq_ref[...] = table.astype(BF16)
    to_time_ref[...] = table.T.astype(BF16)
    size = ROW * ROW
    row = lax.broadcasted_iota(jnp.int32, (size, size), 0)
    column = lax.broadcasted_iota(jnp.int32, (size, size), 1)
    target = lax.rem(row, ROW) * ROW + lax.div(row, ROW)
    swap_ref[...] = jnp.where(column == target, 1.0, 0.0).astype(BF16)


def fold(values):
    rows, lanes = values.shape
    return jnp.sum(values.reshape(rows // 8, 8, lanes), axis=0)


def total(part):
    return jnp.sum(jnp.sum(part, axis=0, keepdims=True), axis=1, keepdims=True)


def dot(a, b):
    return jnp.dot(a, b, preferred_element_type=F32)


def body(members, kern_hbm, rec_hbm, onset_ref,
         first_ref, second_ref, resid_hbm, coef_ref,
         kern, fbuf, rbuf, sbuf, abuf, slot, turned, mid, sums,
         to_time_ref, to_freq_ref, swap_ref,
         kern_sem, slot_sem, out_sem, image_send, image_recv, spec_send, early_recv, last_recv,
         sum_send, sum_recv):
    me = lax.axis_index("freq")
    bins2, receivers, focal = fbuf.shape
    bins = bins2 // 2
    rows_k, rec_local, _ = rbuf.shape
    sources = kern.shape[2]
    blocks = rec_local // ROW
    times = first_ref.shape[1] // ROW
    chunks = 2 if blocks % 2 == 0 else 1
    per_chunk = blocks // chunks
    part = per_chunk * ROW
    others = members - 1
    tile_v = min(256, sources)
    tile_i = min(256, receivers)
    group_k = min(4, rows_k // ROW)
    group_r = 4

    half = members // 2
    side = lax.div(me, half) * half
    place = lax.rem(me, half)

    def near_peers(act):
        @pl.loop(0, half - 1)
        def _(j):
            act(side + lax.rem(place + 1 + j, half))

    def far_peers(act):
        @pl.loop(0, half)
        def _(j):
            act(half - side + lax.rem(place + j, half))

    def all_peers(act):
        near_peers(act)
        far_peers(act)

    def kern_copy(g):
        s = lax.rem(g, DEPTH)
        return pltpu.make_async_copy(kern_hbm.at[:, lax.rem(g, bins)], kern.at[s], kern_sem.at[s])

    def kern_step(g):
        @pl.when(g + DEPTH - 1 < 3 * bins)
        def _():
            kern_copy(g + DEPTH - 1).start()

        kern_copy(g).wait()
        return lax.rem(g, DEPTH)

    def rec_copy(f):
        s = lax.rem(f, 2)
        return pltpu.make_async_copy(rec_hbm.at[:, f], slot.at[s], slot_sem.at[s])

    def resid_in(f):
        s = lax.rem(f, 2)
        return pltpu.make_async_copy(resid_hbm.at[f], slot.at[s], slot_sem.at[s])

    def resid_out(f):
        s = lax.rem(f, 2)
        return pltpu.make_async_copy(slot.at[s], resid_hbm.at[f], out_sem.at[s])

    def wait_bytes(view, sem):
        pltpu.make_async_copy(view, view, sem).wait()

    def image_bytes():
        return rbuf.at[pl.ds(0, others * bins2), pl.ds(0, part), :]

    def spectra_bytes(count, rows):
        return abuf.at[pl.ds(0, count), pl.ds(0, others * rows), :]

    rec_copy(0).start()
    kern_copy(0).start()

    barrier = pltpu.get_barrier_semaphore()

    def greet(to):
        pl.semaphore_signal(barrier, inc=1, device_id={"freq": to}, device_id_type=MESH)

    all_peers(greet)

    lane = lax.broadcasted_iota(jnp.int32, (1, focal), 1)

    def share(turn, parts):
        row = jnp.broadcast_to(total(parts[0]), (1, focal))
        for entry, values in enumerate(parts[1:], 1):
            row = jnp.where(lane < entry, row, total(values))
        sums[turn, me] = row

        def send(to):
            pltpu.make_async_remote_copy(
                src_ref=sums.at[turn, me], dst_ref=sums.at[turn, me],
                send_sem=sum_send.at[turn], recv_sem=sum_recv.at[turn],
                device_id={"freq": to}, device_id_type=MESH,
            ).start()

        all_peers(send)

    def collect(turn, count):
        wait_bytes(sums.at[turn, pl.ds(0, others)], sum_recv.at[turn])
        wait_bytes(sums.at[turn, pl.ds(0, others)], sum_send.at[turn])
        row = jnp.sum(sums[turn], axis=0)
        return [jnp.sum(jnp.where(lane == entry, row, 0.0), axis=1, keepdims=True) for entry in range(count)]

    def send_images(turn, c, first, count):
        def send(to):
            pltpu.make_async_remote_copy(
                src_ref=fbuf.at[pl.ds(first, count), pl.ds(pl.multiple_of(to * rec_local + c * part, ROW), part), :],
                dst_ref=rbuf.at[pl.ds(me * bins2 + first, count), pl.ds(c * part, part), :],
                send_sem=image_send.at[turn], recv_sem=image_recv.at[turn, c],
                device_id={"freq": to}, device_id_type=MESH,
            ).start()

        all_peers(send)

    def send_spectra(peers, turn, first, count, row, rows, recv):
        def send(to):
            pltpu.make_async_remote_copy(
                src_ref=sbuf.at[pl.ds(to * bins2 + first, count), pl.ds(pl.multiple_of(row, ROW), rows), :],
                dst_ref=abuf.at[pl.ds(first, count), pl.ds(pl.multiple_of(me * rec_local + row, ROW), rows), :],
                send_sem=spec_send.at[turn], recv_sem=recv,
                device_id={"freq": to}, device_id_type=MESH,
            ).start()

        peers(send)

    def send_last(turn):
        for peers in (near_peers, far_peers):
            @pl.loop(0, bins)
            def _(f, peers=peers):
                send_spectra(peers, turn, 2 * f, 2, (chunks - 1) * part, part, last_recv.at[turn, f])

    def send_rest(turn):
        for c in range(1, chunks):
            send_images(turn, c, 0, bins2)

    def turn_over(v, real, imag):
        both = jnp.concatenate([real, imag], axis=1)
        turned[:, pl.ds(v * tile_v, tile_v)] = both.T.astype(BF16)

    def images(f, k):
        plain = turned[...]
        cross = jnp.concatenate([plain[focal:], -plain[:focal]], axis=0)
        for i in range(receivers // tile_i):
            cols = pl.ds(i * tile_i, tile_i)
            z = dot(plain, kern[k, 0, :, cols]) + dot(cross, kern[k, 1, :, cols])
            z = z.T.astype(BF16)
            fbuf[2 * f, cols, :] = z[:, :focal]
            fbuf[2 * f + 1, cols, :] = z[:, focal:]
        mine = pl.ds(pl.multiple_of(me * rec_local, ROW), rec_local)
        rbuf[pl.ds(me * bins2 + 2 * f, 2), :, :] = fbuf[pl.ds(2 * f, 2), mine, :]

    def forward(f, k, finish, carry):
        real, imag = abuf[2 * f], abuf[2 * f + 1]
        plain = jnp.concatenate([real, imag], axis=1)
        cross = jnp.concatenate([-imag, real], axis=1)
        for v in range(sources // tile_v):
            rows = pl.ds(v * tile_v, tile_v)
            y = dot(kern[k, 0, rows, :], plain) + dot(kern[k, 1, rows, :], cross)
            carry = finish(v, rows, y[:, :focal], y[:, focal:], carry)
        return carry

    def receivers_side(turn, ib, field, make_field, carry):
        here = pl.ds(pl.multiple_of(ib * ROW, ROW), ROW)

        @pl.when(lax.rem(ib, per_chunk) == 0)
        def _():
            wait_bytes(image_bytes(), image_recv.at[turn, lax.div(ib, per_chunk)])

        @pl.loop(0, rows_k // (ROW * group_k))
        def _(g):
            pieces = []
            for n in range(group_k):
                at = pl.ds((g * group_k + n) * ROW, ROW)
                pieces.append(rbuf[at, here, :].reshape(ROW * ROW, focal))
            out = dot(swap_ref[...], jnp.concatenate(pieces, axis=1)).astype(BF16)
            for n in range(group_k):
                at = pl.ds(pl.multiple_of((g * group_k + n) * ROW, ROW), ROW)
                mid[:, at, :] = out[:, n * focal:(n + 1) * focal].reshape(ROW, ROW, focal)

        steps = lax.broadcasted_iota(jnp.int32, (times, focal), 0)

        def group(g, carry):
            stack = jnp.concatenate([mid[g * group_r + n] for n in range(group_r)], axis=1)
            raw = dot(to_time_ref[...], stack)
            lows = []
            for n in range(group_r):
                r = g * group_r + n
                onset = onset_ref[pl.ds(ib * ROW + r, 1), :]
                kept = jnp.where(steps < onset, raw[:, n * focal:(n + 1) * focal], 0.0)
                kept = make_field(ib, r, kept)
                carry = carry + fold(kept * kept)
                field[ib, pl.ds(r, times, stride=ROW), :] = kept
                lows.append(kept.astype(BF16))
            spec = dot(to_freq_ref[...], jnp.concatenate(lows, axis=1)).astype(BF16)
            for n in range(group_r):
                mid[g * group_r + n] = spec[:, n * focal:(n + 1) * focal]
            return carry

        carry = lax.fori_loop(0, ROW // group_r, group, carry)

        @pl.loop(0, rows_k // (ROW * group_k))
        def _(g):
            pieces = []
            for n in range(group_k):
                at = pl.ds(pl.multiple_of((g * group_k + n) * ROW, ROW), ROW)
                pieces.append(mid[:, at, :].reshape(ROW * ROW, focal))
            out = dot(swap_ref[...], jnp.concatenate(pieces, axis=1)).astype(BF16)
            for n in range(group_k):
                at = pl.ds((g * group_k + n) * ROW, ROW)
                sbuf[at, here, :] = out[:, n * focal:(n + 1) * focal].reshape(ROW, ROW, focal)

        if chunks > 1:
            @pl.when(ib < blocks - per_chunk)
            def _():
                send_spectra(all_peers, turn, 0, bins2, ib * ROW, ROW, early_recv.at[turn])

        start = pl.multiple_of(me * rec_local + ib * ROW, ROW)
        abuf[:, pl.ds(start, ROW), :] = sbuf[pl.ds(me * bins2, bins2), here, :]
        return carry

    zero = jnp.zeros((8, focal), F32)

    def start_step(f, carry):
        @pl.when(f + 1 < bins)
        def _():
            rec_copy(f + 1).start()

        rec_copy(f).wait()

        @pl.when(f == 0)
        def _():
            for g in range(1, DEPTH - 1):
                kern_copy(g).start()

        s = lax.rem(f, 2)
        for v in range(sources // tile_v):
            rows = pl.ds(v * tile_v, tile_v)
            real, imag = slot[s, 0, rows, :], slot[s, 1, rows, :]
            carry = carry + fold(real * real) + fold(imag * imag)
            turn_over(v, real, imag)
        images(f, kern_step(f))

        @pl.when(f == 0)
        def _():
            pl.semaphore_wait(barrier, others)

        send_images(0, 0, 2 * f, 2)
        return carry

    sum_b = lax.fori_loop(0, bins, start_step, zero)
    rec_copy(0).start()
    send_rest(0)
    fill_tables(to_time_ref, to_freq_ref, swap_ref)

    def first_block(ib, carry):
        return receivers_side(0, ib, first_ref, lambda ib, r, kept: kept, carry)

    sum_z = lax.fori_loop(0, blocks, first_block, zero)
    share(0, [sum_b, sum_z])
    send_last(0)
    wait_bytes(fbuf.at[:, pl.ds(0, others * rec_local), :], image_send.at[0])
    square_b, square_z = collect(0, 2)
    beta = jnp.sqrt(square_b)
    image_norm = jnp.sqrt(square_z)
    alpha = image_norm / beta
    scale = 1.0 / image_norm
    weight = alpha / beta

    if chunks > 1:
        wait_bytes(spectra_bytes(bins2, rec_local - part), early_recv.at[0])

    def middle_step(f, carry):
        @pl.when(f >= 1)
        def _():
            resid_out(f - 1).wait()

        @pl.when(f + 1 < bins)
        def _():
            rec_copy(f + 1).start()

        rec_copy(f).wait()
        s = lax.rem(f, 2)

        def finish(v, rows, real, imag, carry):
            real = real * scale - weight * slot[s, 0, rows, :]
            imag = imag * scale - weight * slot[s, 1, rows, :]
            slot[s, 0, rows, :] = real
            slot[s, 1, rows, :] = imag
            turn_over(v, real, imag)
            return carry + fold(real * real) + fold(imag * imag)

        wait_bytes(spectra_bytes(2, part), last_recv.at[0, f])
        k = kern_step(bins + f)
        carry = forward(f, k, finish, carry)
        resid_out(f).start()
        images(f, k)
        send_images(1, 0, 2 * f, 2)
        return carry

    sum_u = lax.fori_loop(0, bins, middle_step, zero)
    share(1, [sum_u])
    send_rest(1)
    resid_out(bins - 1).wait()
    resid_in(0).start()
    (square_u,) = collect(1, 1)
    beta_u = jnp.sqrt(square_u)
    data_scale = 1.0 / beta_u
    back = beta_u * scale

    wait_bytes(sbuf.at[pl.ds(0, others * bins2)], spec_send.at[0])

    def second_block(ib, carry):
        def make_field(ib, r, kept):
            return kept * data_scale - back * first_ref[ib, pl.ds(r, times, stride=ROW), :]

        return receivers_side(1, ib, second_ref, make_field, carry)

    sum_v = lax.fori_loop(0, blocks, second_block, zero)
    share(2, [sum_v])
    send_last(1)
    (square_v,) = collect(2, 1)
    alpha_v = jnp.sqrt(square_v)
    last_scale = 1.0 / alpha_v
    last_weight = alpha_v * data_scale

    if chunks > 1:
        wait_bytes(spectra_bytes(bins2, rec_local - part), early_recv.at[1])

    def last_step(f, carry):
        @pl.when(f + 1 < bins)
        def _():
            resid_in(f + 1).start()

        resid_in(f).wait()
        s = lax.rem(f, 2)

        def finish(v, rows, real, imag, carry):
            real = real * last_scale - last_weight * slot[s, 0, rows, :]
            imag = imag * last_scale - last_weight * slot[s, 1, rows, :]
            return carry + fold(real * real) + fold(imag * imag)

        wait_bytes(spectra_bytes(2, part), last_recv.at[1, f])
        return forward(f, kern_step(2 * bins + f), finish, carry)

    sum_last = lax.fori_loop(0, bins, last_step, zero)
    share(3, [sum_last])

    wait_bytes(fbuf.at[:, pl.ds(0, others * rec_local), :], image_send.at[1])
    wait_bytes(sbuf.at[pl.ds(0, others * bins2)], spec_send.at[1])

    (square_last,) = collect(3, 1)

    rho = jnp.sqrt(alpha * alpha + square_u)
    cosine, sine = alpha / rho, beta_u / rho
    phi = cosine * beta
    phibar = sine * beta
    theta = sine * alpha_v
    rhobar = -cosine * alpha_v
    rho_last = jnp.sqrt(rhobar * rhobar + square_last)
    step_last = rhobar / rho_last * phibar / rho_last
    on_first = (phi / rho - step_last * theta / rho) * scale
    on_second = step_last * last_scale
    coef_ref[0] = jnp.broadcast_to(on_first, (8, focal))
    coef_ref[1] = jnp.broadcast_to(on_second, (8, focal))


def weigh(coef_ref, first_ref, second_ref, out_hbm, held, sem):
    pieces, span = held.shape[0], held.shape[1]
    blocks, _, focal = first_ref.shape
    on_first, on_second = coef_ref[0, 0:1, :], coef_ref[1, 0:1, :]

    def write(n):
        return pltpu.make_async_copy(held.at[n], out_hbm.at[pl.ds(n * span, span)], sem.at[n])

    @pl.loop(0, pieces)
    def _(n):
        rows = pl.ds(pl.multiple_of(n * span * ROW, ROW), span * ROW)
        for ib in range(blocks):
            both = on_first * first_ref[ib, rows, :] + on_second * second_ref[ib, rows, :]
            held[n, :, ib * ROW:(ib + 1) * ROW, :] = both.reshape(span, ROW, focal)
        write(n).start()

    @pl.loop(0, pieces)
    def _(n):
        write(n).wait()


def make_step(mesh):
    members = mesh.shape["freq"]

    def step(kernel, recorded, onset_time):
        _, bins, sources, receivers = kernel.shape
        rec_local, focal = onset_time.shape
        times = 2 * bins * members
        blocks = rec_local // ROW
        hbm = pl.BlockSpec(memory_space=pltpu.HBM)
        vmem = pl.BlockSpec(memory_space=pltpu.VMEM)
        shape = jax.ShapeDtypeStruct
        first, second, _, coef = pl.pallas_call(
            functools.partial(body, members),
            out_shape=(
                shape((blocks, times * ROW, focal), F32),
                shape((blocks, times * ROW, focal), F32),
                shape((bins, 2, sources, focal), F32),
                shape((2, 8, focal), F32),
            ),
            in_specs=[hbm, hbm, vmem],
            out_specs=(vmem, vmem, hbm, vmem),
            scratch_shapes=[
                pltpu.VMEM((DEPTH, 2, sources, receivers), BF16),
                pltpu.VMEM((2 * bins, receivers, focal), BF16),
                pltpu.VMEM((times, rec_local, focal), BF16),
                pltpu.VMEM((times, rec_local, focal), BF16),
                pltpu.VMEM((2 * bins, receivers, focal), BF16),
                pltpu.VMEM((2, 2, sources, focal), F32),
                pltpu.VMEM((2 * focal, sources), BF16),
                pltpu.VMEM((ROW, times, focal), BF16),
                pltpu.VMEM((4, members, 1, focal), F32),
                pltpu.VMEM((times, times), BF16),
                pltpu.VMEM((times, times), BF16),
                pltpu.VMEM((ROW * ROW, ROW * ROW), BF16),
                pltpu.SemaphoreType.DMA((DEPTH,)),
                pltpu.SemaphoreType.DMA((2,)),
                pltpu.SemaphoreType.DMA((2,)),
                pltpu.SemaphoreType.DMA((2,)),
                pltpu.SemaphoreType.DMA((2, 2)),
                pltpu.SemaphoreType.DMA((2,)),
                pltpu.SemaphoreType.DMA((2,)),
                pltpu.SemaphoreType.DMA((2, bins)),
                pltpu.SemaphoreType.DMA((4,)),
                pltpu.SemaphoreType.DMA((4,)),
            ],
            compiler_params=pltpu.CompilerParams(
                collective_id=0, has_side_effects=True, vmem_limit_bytes=VMEM_MAIN
            ),
            name="lsqr",
        )(kernel, recorded, onset_time)
        pieces = 16
        span = times // pieces
        return pl.pallas_call(
            weigh,
            out_shape=shape((times, rec_local, focal), F32),
            in_specs=[vmem, vmem, vmem],
            out_specs=hbm,
            scratch_shapes=[
                pltpu.VMEM((pieces, span, rec_local, focal), F32),
                pltpu.SemaphoreType.DMA((pieces,)),
            ],
            compiler_params=pltpu.CompilerParams(vmem_limit_bytes=VMEM_WEIGH),
            name="weigh",
        )(coef, first, second)

    return step


def solution(mesh):
    placed = (
        P(None, ("grp", "freq"), None, None),
        P(None, ("grp", "freq"), None, None),
        P(("grp", "freq"), None),
    )
    return jax.shard_map(
        make_step(mesh), mesh=mesh, in_specs=placed, out_specs=P(None, ("grp", "freq"), None), check_vma=False
    )
```
